512 devices in a mesh: gx: 64 (over x, y, core), ta: 8 (over z).
Axes of the slice: x: 4, y: 8, z: 8, core: 2. Of those that a mesh axis runs over, the one named last changes fastest.
Arguments:
- master_flat: float32 [8388608], P(('gx', 'ta')), may hold values from -6 to 6
Outputs:
- serving_weight: bfloat16 [1, 8192, 1024], P(None, None, 'ta')
- channel_scale: float32 [1, 1024], P(None, 'ta')
The draws below stay inside these ranges and needn't reach their ends.
All inputs are finite; a program needn't handle non-finite values.
Results may differ from the reference program's by a relative error of at most 0.015.
Values may be sent and summed in bfloat16 or wider, within the bound.
A program may use at most 64 MiB of HBM per device.

```python
import jax
import jax.numpy as jnp

D = 8192
KVH = 8
HEAD = 128
LAYERS = 1


def level_of(own_key, dims, split, least, top_value):
    factor_of, own = 1.0, jax.random.fold_in(own_key, 6)
    for axis_at, blocks in split:
        steps = jnp.exp(jax.random.uniform(jax.random.fold_in(own, axis_at), (blocks,), jnp.float32, least / len(split), top_value / len(split)))
        factor_of = factor_of * jnp.repeat(steps, dims[axis_at] // blocks).reshape([-1 if axis == axis_at else 1 for axis in range(len(dims))])
    return factor_of


def gaussian(key, shape, deviation, bound, cuts=(), kind=jnp.bfloat16):
    level = level_of(key, shape, cuts, -0.22, 0.18) if cuts else 1.0
    values = jax.random.normal(key, shape, jnp.float32) * deviation * level
    return jnp.minimum(jnp.maximum(values, -bound), bound).astype(kind)


def setup_inputs(seed: int = 0) -> dict:
    seeds = jax.random.split(jax.random.key(seed), 2)
    return {
        "master_flat": gaussian(seeds[0], (LAYERS * D * KVH * HEAD,), 1.0, 6.0, ((0, 512),), jnp.float32),
    }


def reference(master_flat):
    weight = master_flat.reshape(LAYERS, D, KVH * HEAD).astype(jnp.bfloat16)
    wide = weight.astype(jnp.float32)
    channel_scale = jnp.max(jnp.abs(wide), axis=1)
    serving_weight = (wide / channel_scale[:, None, :]).astype(jnp.bfloat16)
    return serving_weight, channel_scale
```

```python
import functools

import jax
import jax.numpy as jnp
from jax import lax
from jax.experimental import pallas as pl
from jax.experimental.pallas import tpu as pltpu
from jax.sharding import PartitionSpec as P

D = 8192
HEADS_WIDTH = 128
X, Y, Z = 4, 8, 8
ROWS = 16
HALF = Z * ROWS
FIRST = 3 * ROWS
MESH = pl.DeviceIdType.MESH


def order_of(step, size):
    return lax.rem(jnp.where(step % 2 == 1, (step + 1) // 2, size - step // 2), size)


def gather_kernel(x_hbm, out_ref, stage, rounded, load_sem, swap_send, swap_recv, send_sem, a_recv, b_recv, core_send, core_recv):
    gx, z = lax.axis_index("gx"), lax.axis_index("ta")
    core, chip = lax.rem(gx, 2), gx // 2
    x, y = chip // Y, lax.rem(chip, Y)

    load = pltpu.make_async_copy(x_hbm, stage, load_sem)
    load.start()

    barrier = pltpu.get_barrier_semaphore()

    def device(xt, yt, zt, ct):
        return ((xt * Y + yt) * 2 + ct, zt)

    def greet(xt, yt, zt, ct):
        pl.semaphore_signal(barrier, inc=1, device_id=device(xt, yt, zt, ct), device_id_type=MESH)

    greet(x, y, z, 1 - core)
    for d in range(1, Z):
        greet(x, y, lax.rem(z + d, Z), core)
    for d in range(1, Y):
        greet(x, lax.rem(y + d, Y), z, core)
    for d in range(1, X):
        greet(lax.rem(x + d, X), y, z, core)

    def rows_of(xt, yt, ct, offset, count):
        start = ((xt * Y + yt) * 2 + ct) * HALF + offset
        return pl.ds(pl.multiple_of(start, ROWS), count)

    load.wait()
    for k in range(Z):
        rounded[k] = stage[pl.ds(k, ROWS, stride=Z), :].astype(jnp.bfloat16)
    out_ref[rows_of(x, y, core, z * ROWS, ROWS), :] = rounded[z]

    pl.semaphore_wait(barrier, 1 + (Z - 1) + (Y - 1) + (X - 1))

    def remote(src, dst, send, recv, to):
        return pltpu.make_async_remote_copy(src_ref=src, dst_ref=dst, send_sem=send, recv_sem=recv, device_id=to, device_id_type=MESH)

    here = out_ref.at[rows_of(x, y, core, z * ROWS, ROWS)]
    for d in (4, 3, 5, 2, 6, 1, 7):
        to = lax.rem(z + d, Z)
        remote(rounded.at[to], here, swap_send, swap_recv, device(x, y, to, core)).start()

    def along_y(ref, recv):
        for d in (4, 3, 5, 2, 6, 1, 7):
            remote(ref, ref, send_sem, recv, device(x, lax.rem(y + d, Y), z, core)).start()

    def along_x(ref, recv):
        for d in (2, 1, 3):
            remote(ref, ref, send_sem, recv, device(lax.rem(x + d, X), y, z, core)).start()

    def across(ref):
        remote(ref, ref, core_send, core_recv, device(x, y, z, 1 - core)).start()

    def part_a(xt, yt):
        return out_ref.at[rows_of(xt, yt, core, 0, FIRST)]

    def part_b(xt, yt):
        return out_ref.at[rows_of(xt, yt, core, FIRST, HALF - FIRST)]

    def whole(xt, yt):
        return out_ref.at[rows_of(xt, yt, core, 0, HALF)]

    def waiter(ref, sem):
        pltpu.make_async_copy(ref, ref, sem).wait()

    others = out_ref.at[pl.ds(0, (Z - 1) * ROWS)]
    waiter(others, swap_recv)
    along_x(part_a(x, y), a_recv.at[chip])
    along_y(part_b(x, y), b_recv.at[chip])
    along_y(part_a(x, y), a_recv.at[chip])
    along_x(part_b(x, y), b_recv.at[chip])
    across(whole(x, y))

    def arrival(step, carry):
        xt = order_of(step // 8, X)
        yt = order_of(lax.rem(step, 8), Y)
        source = xt * Y + yt

        @pl.when(source != chip)
        def _():
            waiter(part_a(xt, yt), a_recv.at[source])

            @pl.when(yt == y)
            def _():
                along_y(part_a(xt, yt), a_recv.at[source])

            waiter(part_b(xt, yt), b_recv.at[source])

            @pl.when(xt == x)
            def _():
                along_x(part_b(xt, yt), b_recv.at[source])

            across(whole(xt, yt))

        return carry

    lax.fori_loop(0, X * Y, arrival, 0)

    waiter(out_ref.at[pl.ds(0, D // 2)], core_recv)
    waiter(others, swap_send)
    sent = X * FIRST * (Y - 1) + (X - 1) * FIRST + Y * (HALF - FIRST) * (X - 1) + (Y - 1) * (HALF - FIRST)
    waiter(out_ref.at[pl.ds(0, sent)], send_sem)
    waiter(out_ref.at[pl.ds(0, D // 2)], core_send)


TILE = 1024


def scale_kernel(w_ref, out_hbm, scale_hbm, buffer, scale_vmem, out_sem, scale_sem):
    def step(i, best):
        block = jnp.abs(w_ref[pl.ds(pl.multiple_of(i * 256, 256), 256), :])
        return jnp.maximum(best, jnp.max(block.reshape(8, 32, HEADS_WIDTH), axis=0))

    best = lax.fori_loop(0, D // 256, step, jnp.zeros((32, HEADS_WIDTH), jnp.bfloat16))
    scale = jnp.max(best.astype(jnp.float32), axis=0, keepdims=True)
    scale_vmem[...] = scale
    scale_out = pltpu.make_async_copy(scale_vmem, scale_hbm, scale_sem)
    scale_out.start()
    inverse = jnp.broadcast_to(1.0 / scale, (64, HEADS_WIDTH))
    copies = []
    for t in range(D // TILE):
        def scaled(i, carry):
            rows = pl.ds(pl.multiple_of(t * TILE + i * 64, 64), 64)
            buffer[rows, :] = (w_ref[rows, :].astype(jnp.float32) * inverse).astype(jnp.bfloat16)
            return carry

        lax.fori_loop(0, TILE // 64, scaled, 0, unroll=4)
        rows = pl.ds(t * TILE, TILE)
        copies.append(pltpu.make_async_copy(buffer.at[rows], out_hbm.at[rows], out_sem.at[t]))
        copies[-1].start()
    for copy in copies:
        copy.wait()
    scale_out.wait()


def shards(master_flat):
    flat = master_flat.reshape(ROWS * Z, HEADS_WIDTH)
    gathered = pl.pallas_call(
        gather_kernel,
        name="gather",
        out_shape=jax.ShapeDtypeStruct((D, HEADS_WIDTH), jnp.bfloat16),
        in_specs=[pl.BlockSpec(memory_space=pltpu.HBM)],
        out_specs=pl.BlockSpec(memory_space=pltpu.VMEM),
        scratch_shapes=[
            pltpu.VMEM((ROWS * Z, HEADS_WIDTH), jnp.float32),
            pltpu.VMEM((Z, ROWS, HEADS_WIDTH), jnp.bfloat16),
            pltpu.SemaphoreType.DMA,
            pltpu.SemaphoreType.DMA,
            pltpu.SemaphoreType.DMA,
            pltpu.SemaphoreType.DMA,
            pltpu.SemaphoreType.DMA((X * Y,)),
            pltpu.SemaphoreType.DMA((X * Y,)),
            pltpu.SemaphoreType.DMA,
            pltpu.SemaphoreType.DMA,
        ],
        compiler_params=pltpu.CompilerParams(collective_id=0, has_side_effects=True, vmem_limit_bytes=16 * 1024 * 1024),
    )(flat)
    weight, scale = pl.pallas_call(
        scale_kernel,
        name="scale",
        out_shape=(jax.ShapeDtypeStruct((D, HEADS_WIDTH), jnp.bfloat16), jax.ShapeDtypeStruct((1, HEADS_WIDTH), jnp.float32)),
        in_specs=[pl.BlockSpec(memory_space=pltpu.VMEM)],
        out_specs=(pl.BlockSpec(memory_space=pl.ANY), pl.BlockSpec(memory_space=pl.ANY)),
        scratch_shapes=[
            pltpu.VMEM((D, HEADS_WIDTH), jnp.bfloat16),
            pltpu.VMEM((1, HEADS_WIDTH), jnp.float32),
            pltpu.SemaphoreType.DMA((D // TILE,)),
            pltpu.SemaphoreType.DMA,
        ],
        compiler_params=pltpu.CompilerParams(vmem_limit_bytes=16 * 1024 * 1024),
    )(gathered)
    return weight.reshape(1, D, HEADS_WIDTH), scale


def solution(mesh):
    return jax.shard_map(shards, mesh=mesh, in_specs=(P(("gx", "ta")),), out_specs=(P(None, None, "ta"), P(None, "ta")), check_vma=False)
```

```python
import functools

import jax
import jax.numpy as jnp
from jax import lax
from jax.experimental import pallas as pl
from jax.experimental.pallas import tpu as pltpu
from jax.sharding import PartitionSpec as P

D = 8192
HEADS_WIDTH = 128
X, Y, Z = 4, 8, 8
ROWS = 16
HALF = Z * ROWS
FIRST = 2 * ROWS
MESH = pl.DeviceIdType.MESH


def order_of(step, size):
    return lax.rem(jnp.where(step % 2 == 1, (step + 1) // 2, size - step // 2), size)


def gather_kernel(x_hbm, out_ref, stage, rounded, load_sem, swap_send, swap_recv, send_sem, a_recv, b_recv, core_send, core_recv):
    gx, z = lax.axis_index("gx"), lax.axis_index("ta")
    core, chip = lax.rem(gx, 2), gx // 2
    x, y = chip // Y, lax.rem(chip, Y)

    load = pltpu.make_async_copy(x_hbm, stage, load_sem)
    load.start()

    barrier = pltpu.get_barrier_semaphore()

    def device(xt, yt, zt, ct):
        return ((xt * Y + yt) * 2 + ct, zt)

    def greet(xt, yt, zt, ct):
        pl.semaphore_signal(barrier, inc=1, device_id=device(xt, yt, zt, ct), device_id_type=MESH)

    greet(x, y, z, 1 - core)
    for d in range(1, Z):
        greet(x, y, lax.rem(z + d, Z), core)
    for d in range(1, Y):
        greet(x, lax.rem(y + d, Y), z, core)
    for d in range(1, X):
        greet(lax.rem(x + d, X), y, z, core)

    def rows_of(xt, yt, ct, offset, count):
        start = ((xt * Y + yt) * 2 + ct) * HALF + offset
        return pl.ds(pl.multiple_of(start, ROWS), count)

    load.wait()
    for k in range(Z):
        rounded[k] = stage[pl.ds(k, ROWS, stride=Z), :].astype(jnp.bfloat16)
    out_ref[rows_of(x, y, core, z * ROWS, ROWS), :] = rounded[z]

    pl.semaphore_wait(barrier, 1 + (Z - 1) + (Y - 1) + (X - 1))

    def remote(src, dst, send, recv, to):
        return pltpu.make_async_remote_copy(src_ref=src, dst_ref=dst, send_sem=send, recv_sem=recv, device_id=to, device_id_type=MESH)

    here = out_ref.at[rows_of(x, y, core, z * ROWS, ROWS)]
    for d in (4, 3, 5, 2, 6, 1, 7):
        to = lax.rem(z + d, Z)
        remote(rounded.at[to], here, swap_send, swap_recv, device(x, y, to, core)).start()

    def along_y(ref, recv):
        for d in (4, 3, 5, 2, 6, 1, 7):
            remote(ref, ref, send_sem, recv, device(x, lax.rem(y + d, Y), z, core)).start()

    def along_x(ref, recv):
        for d in (2, 1, 3):
            remote(ref, ref, send_sem, recv, device(lax.rem(x + d, X), y, z, core)).start()

    def across(ref):
        remote(ref, ref, core_send, core_recv, device(x, y, z, 1 - core)).start()

    def part_a(xt, yt):
        return out_ref.at[rows_of(xt, yt, core, 0, FIRST)]

    def part_b(xt, yt):
        return out_ref.at[rows_of(xt, yt, core, FIRST, HALF - FIRST)]

    def whole(xt, yt):
        return out_ref.at[rows_of(xt, yt, core, 0, HALF)]

    def waiter(ref, sem):
        pltpu.make_async_copy(ref, ref, sem).wait()

    others = out_ref.at[pl.ds(0, (Z - 1) * ROWS)]
    waiter(others, swap_recv)
    along_x(part_a(x, y), a_recv.at[chip])
    along_y(part_b(x, y), b_recv.at[chip])
    along_y(part_a(x, y), a_recv.at[chip])
    along_x(part_b(x, y), b_recv.at[chip])
    across(whole(x, y))

    def from_x(step, carry):
        xt = order_of(step, X)

        @pl.when(xt != x)
        def _():
            source = xt * Y + y
            waiter(part_a(xt, y), a_recv.at[source])
            along_y(part_a(xt, y), a_recv.at[source])

        return carry

    def from_y(step, carry):
        yt = order_of(step, Y)

        @pl.when(yt != y)
        def _():
            source = x * Y + yt
            waiter(part_b(x, yt), b_recv.at[source])
            along_x(part_b(x, yt), b_recv.at[source])

        return carry

    lax.fori_loop(0, 2, from_y, 0)
    lax.fori_loop(0, 2, from_x, 0)
    lax.fori_loop(2, 5, from_y, 0)
    lax.fori_loop(2, X, from_x, 0)
    lax.fori_loop(5, Y, from_y, 0)

    def arrival(step, carry):
        xt = order_of(step // 8, X)
        yt = order_of(lax.rem(step, 8), Y)
        source = xt * Y + yt

        @pl.when(source != chip)
        def _():
            @pl.when(yt != y)
            def _():
                waiter(part_a(xt, yt), a_recv.at[source])

            @pl.when(xt != x)
            def _():
                waiter(part_b(xt, yt), b_recv.at[source])

            across(whole(xt, yt))

        return carry

    lax.fori_loop(0, X * Y, arrival, 0)

    waiter(out_ref.at[pl.ds(0, D // 2)], core_recv)
    waiter(others, swap_send)
    sent = X * FIRST * (Y - 1) + (X - 1) * FIRST + Y * (HALF - FIRST) * (X - 1) + (Y - 1) * (HALF - FIRST)
    waiter(out_ref.at[pl.ds(0, sent)], send_sem)
    waiter(out_ref.at[pl.ds(0, D // 2)], core_send)


TILE = 1024


def scale_kernel(w_ref, out_hbm, scale_hbm, buffer, scale_vmem, out_sem, scale_sem):
    def step(i, best):
        block = jnp.abs(w_ref[pl.ds(pl.multiple_of(i * 256, 256), 256), :])
        return jnp.maximum(best, jnp.max(block.reshape(8, 32, HEADS_WIDTH), axis=0))

    best = lax.fori_loop(0, D // 256, step, jnp.zeros((32, HEADS_WIDTH), jnp.bfloat16))
    scale = jnp.max(best.astype(jnp.float32), axis=0, keepdims=True)
    scale_vmem[...] = scale
    scale_out = pltpu.make_async_copy(scale_vmem, scale_hbm, scale_sem)
    scale_out.start()
    inverse = jnp.broadcast_to(1.0 / scale, (64, HEADS_WIDTH))
    copies = []
    for t in range(D // TILE):
        def scaled(i, carry):
            rows = pl.ds(pl.multiple_of(t * TILE + i * 64, 64), 64)
            buffer[rows, :] = (w_ref[rows, :].astype(jnp.float32) * inverse).astype(jnp.bfloat16)
            return carry

        lax.fori_loop(0, TILE // 64, scaled, 0, unroll=4)
        rows = pl.ds(t * TILE, TILE)
        copies.append(pltpu.make_async_copy(buffer.at[rows], out_hbm.at[rows], out_sem.at[t]))
        copies[-1].start()
    for copy in copies:
        copy.wait()
    scale_out.wait()


def shards(master_flat):
    flat = pltpu.with_memory_space_constraint(master_flat.reshape(ROWS * Z, HEADS_WIDTH), pltpu.HBM)
    gathered = pl.pallas_call(
        gather_kernel,
        name="gather",
        out_shape=jax.ShapeDtypeStruct((D, HEADS_WIDTH), jnp.bfloat16),
        in_specs=[pl.BlockSpec(memory_space=pltpu.HBM)],
        out_specs=pl.BlockSpec(memory_space=pltpu.VMEM),
        scratch_shapes=[
            pltpu.VMEM((ROWS * Z, HEADS_WIDTH), jnp.float32),
            pltpu.VMEM((Z, ROWS, HEADS_WIDTH), jnp.bfloat16),
            pltpu.SemaphoreType.DMA,
            pltpu.SemaphoreType.DMA,
            pltpu.SemaphoreType.DMA,
            pltpu.SemaphoreType.DMA,
            pltpu.SemaphoreType.DMA((X * Y,)),
            pltpu.SemaphoreType.DMA((X * Y,)),
            pltpu.SemaphoreType.DMA,
            pltpu.SemaphoreType.DMA,
        ],
        compiler_params=pltpu.CompilerParams(collective_id=0, has_side_effects=True, vmem_limit_bytes=16 * 1024 * 1024),
    )(flat)
    weight, scale = pl.pallas_call(
        scale_kernel,
        name="scale",
        out_shape=(jax.ShapeDtypeStruct((D, HEADS_WIDTH), jnp.bfloat16), jax.ShapeDtypeStruct((1, HEADS_WIDTH), jnp.float32)),
        in_specs=[pl.BlockSpec(memory_space=pltpu.VMEM)],
        out_specs=(pl.BlockSpec(memory_space=pl.ANY), pl.BlockSpec(memory_space=pl.ANY)),
        scratch_shapes=[
            pltpu.VMEM((D, HEADS_WIDTH), jnp.bfloat16),
            pltpu.VMEM((1, HEADS_WIDTH), jnp.float32),
            pltpu.SemaphoreType.DMA((D // TILE,)),
            pltpu.SemaphoreType.DMA,
        ],
        compiler_params=pltpu.CompilerParams(vmem_limit_bytes=16 * 1024 * 1024),
    )(gathered)
    return weight.reshape(1, D, HEADS_WIDTH), scale


def solution(mesh):
    return jax.shard_map(shards, mesh=mesh, in_specs=(P(("gx", "ta")),), out_specs=(P(None, None, "ta"), P(None, "ta")), check_vma=False)
```

```python
import functools

import jax
import jax.numpy as jnp
from jax import lax
from jax.experimental import pallas as pl
from jax.experimental.pallas import tpu as pltpu
from jax.sharding import PartitionSpec as P

D = 8192
HEADS_WIDTH = 128
X, Y, Z = 4, 8, 8
ROWS = 16
HALF = Z * ROWS
A_END, LATE = 2, 5
MESH = pl.DeviceIdType.MESH


def rank(at, size):
    return jnp.where(at * 2 <= size, jnp.maximum(2 * at - 1, 0), 2 * (size - at))


def order_of(step, size):
    return lax.rem(jnp.where(step % 2 == 1, (step + 1) // 2, size - step // 2), size)


def gather_kernel(x_hbm, out_ref, stage, rounded, load_sem, entered_z, entered, swap_send, swap_recv, send_sem, a_recv, b_recv, late_recv, core_send, core_recv):
    gx, z = lax.axis_index("gx"), lax.axis_index("ta")
    core, chip = lax.rem(gx, 2), gx // 2
    x, y = chip // Y, lax.rem(chip, Y)
    x_rank, y_rank = rank(x, X), rank(y, Y)

    load = pltpu.make_async_copy(x_hbm, stage, load_sem)
    load.start()

    barrier = pltpu.get_barrier_semaphore()

    def device(xt, yt, zt, ct):
        return ((xt * Y + yt) * 2 + ct, zt)

    def signal(semaphore, to):
        pl.semaphore_signal(semaphore, inc=1, device_id=to, device_id_type=MESH)

    def around(size, at, then):
        for d in range(1, size):
            then(lax.rem(at + d, size))

    def greet(later, to):
        @pl.when(later)
        def _():
            signal(barrier, to)

    greet(core == 1, device(x, y, z, 1 - core))
    around(Z, z, lambda zt: greet(zt > z, device(x, y, zt, core)))
    around(Y, y, lambda yt: greet(rank(yt, Y) > y_rank, device(x, yt, z, core)))
    around(X, x, lambda xt: greet(rank(xt, X) > x_rank, device(xt, y, z, core)))

    def rows_of(xt, yt, ct, offset, count):
        start = ((xt * Y + yt) * 2 + ct) * HALF + offset
        return pl.ds(pl.multiple_of(start, ROWS), count)

    def wait_for(semaphore, count):
        @pl.when(count > 0)
        def _():
            pl.semaphore_wait(semaphore, count)

    wait_for(barrier, (1 - core) + z + y_rank + x_rank)

    def answer(earlier, semaphore, to):
        @pl.when(earlier)
        def _():
            signal(semaphore, to)

    around(Z, z, lambda zt: answer(zt < z, entered_z.at[z], device(x, y, zt, core)))
    around(Y, y, lambda yt: answer(rank(yt, Y) < y_rank, entered, device(x, yt, z, core)))
    around(X, x, lambda xt: answer(rank(xt, X) < x_rank, entered, device(xt, y, z, core)))
    answer(core == 0, entered, device(x, y, z, 1 - core))

    load.wait()
    for k in range(Z):
        rounded[k] = stage[pl.ds(k, ROWS, stride=Z), :].astype(jnp.bfloat16)
    here = rows_of(x, y, core, z * ROWS, ROWS)
    out_ref[here, :] = rounded[z]

    def remote(src, dst, send, recv, to):
        return pltpu.make_async_remote_copy(src_ref=src, dst_ref=dst, send_sem=send, recv_sem=recv, device_id=to, device_id_type=MESH)

    def swap(zt):
        @pl.when(zt > z)
        def _():
            pl.semaphore_wait(entered_z.at[zt], 1)

        remote(rounded.at[zt], out_ref.at[here], swap_send, swap_recv.at[z], device(x, y, zt, core)).start()

    def swap_soon(zt, carry):
        @pl.when((zt != z) & ((zt < z) | (zt < LATE)))
        def _():
            swap(zt)

        return carry

    def swap_rest(zt, carry):
        @pl.when(zt > z)
        def _():
            swap(zt)

        return carry

    def waiter(ref, sem):
        pltpu.make_async_copy(ref, ref, sem).wait()

    def swapped(zt, carry):
        @pl.when(zt != z)
        def _():
            waiter(rounded.at[zt], swap_recv.at[zt])

        return carry

    def along_y(ref, recv):
        for d in (4, 3, 5, 2, 6, 1, 7):
            remote(ref, ref, send_sem, recv, device(x, lax.rem(y + d, Y), z, core)).start()

    def along_x(ref, recv):
        for d in (2, 1, 3):
            remote(ref, ref, send_sem, recv, device(lax.rem(x + d, X), y, z, core)).start()

    def across(ref):
        remote(ref, ref, core_send, core_recv, device(x, y, z, 1 - core)).start()

    def part_a(xt, yt):
        return out_ref.at[rows_of(xt, yt, core, 0, A_END * ROWS)]

    def part_b(xt, yt):
        return out_ref.at[rows_of(xt, yt, core, A_END * ROWS, (LATE - A_END) * ROWS)]

    def part_late(xt, yt):
        return out_ref.at[rows_of(xt, yt, core, LATE * ROWS, (Z - LATE) * ROWS)]

    def early(xt, yt):
        return out_ref.at[rows_of(xt, yt, core, 0, LATE * ROWS)]

    lax.fori_loop(0, Z, swap_soon, 0)
    lax.fori_loop(0, A_END, swapped, 0)
    wait_for(entered, (Y - 1 - y_rank) + (X - 1 - x_rank) + core)
    along_x(part_a(x, y), a_recv.at[chip])
    along_y(part_a(x, y), a_recv.at[chip])
    lax.fori_loop(A_END, LATE, swapped, 0)
    along_y(part_b(x, y), b_recv.at[chip])
    along_x(part_b(x, y), b_recv.at[chip])
    across(early(x, y))
    lax.fori_loop(LATE, Z, swap_rest, 0)
    lax.fori_loop(LATE, Z, swapped, 0)
    along_y(part_late(x, y), late_recv.at[chip])
    along_x(part_late(x, y), late_recv.at[chip])
    across(part_late(x, y))

    def forward(part, recv, step, over_x):
        xt, yt = (order_of(step, X), y) if over_x else (x, order_of(step, Y))

        @pl.when((xt != x) | (yt != y))
        def _():
            ref, sem = part(xt, yt), recv.at[xt * Y + yt]
            waiter(ref, sem)
            (along_y if over_x else along_x)(ref, sem)

        return 0

    from_x = lambda step, carry: forward(part_a, a_recv, step, True)
    from_y = lambda step, carry: forward(part_b, b_recv, step, False)
    late_from_y = lambda step, carry: forward(part_late, late_recv, step, False)
    lax.fori_loop(0, X, from_x, 0)
    lax.fori_loop(0, Y, from_y, 0)
    lax.fori_loop(0, Y, late_from_y, 0)

    def arrival(step, carry):
        xt, yt = order_of(step // 8, X), order_of(lax.rem(step, 8), Y)
        source = xt * Y + yt

        @pl.when(source != chip)
        def _():
            @pl.when(yt != y)
            def _():
                waiter(part_a(xt, yt), a_recv.at[source])

            @pl.when(xt != x)
            def _():
                waiter(part_b(xt, yt), b_recv.at[source])

            across(early(xt, yt))

        return carry

    def late_arrival(step, carry):
        xt, yt = order_of(step // 8, X), order_of(lax.rem(step, 8), Y)
        source = xt * Y + yt

        @pl.when(source != chip)
        def _():
            @pl.when(xt != x)
            def _():
                waiter(part_late(xt, yt), late_recv.at[source])

            across(part_late(xt, yt))

        return carry

    lax.fori_loop(0, X * Y, arrival, 0)
    lax.fori_loop(0, X * Y, late_arrival, 0)

    waiter(out_ref.at[pl.ds(0, D // 2)], core_recv)
    waiter(out_ref.at[pl.ds(0, (Z - 1) * ROWS)], swap_send)
    a_rows, b_rows = A_END * ROWS, (Z - A_END) * ROWS
    sent = a_rows * ((X - 1) + X * (Y - 1)) + b_rows * ((Y - 1) + Y * (X - 1))
    waiter(out_ref.at[pl.ds(0, sent)], send_sem)
    waiter(out_ref.at[pl.ds(0, D // 2)], core_send)


TILE = 1024


def scale_kernel(w_ref, out_hbm, scale_hbm, buffer, scale_vmem, out_sem, scale_sem):
    def step(i, best):
        block = jnp.abs(w_ref[pl.ds(pl.multiple_of(i * 256, 256), 256), :])
        return jnp.maximum(best, jnp.max(block.reshape(8, 32, HEADS_WIDTH), axis=0))

    best = lax.fori_loop(0, D // 256, step, jnp.zeros((32, HEADS_WIDTH), jnp.bfloat16))
    scale = jnp.max(best.astype(jnp.float32), axis=0, keepdims=True)
    scale_vmem[...] = scale
    scale_out = pltpu.make_async_copy(scale_vmem, scale_hbm, scale_sem)
    scale_out.start()
    inverse = jnp.broadcast_to(1.0 / scale, (64, HEADS_WIDTH))
    copies = []
    for t in range(D // TILE):
        def scaled(i, carry):
            rows = pl.ds(pl.multiple_of(t * TILE + i * 64, 64), 64)
            buffer[rows, :] = (w_ref[rows, :].astype(jnp.float32) * inverse).astype(jnp.bfloat16)
            return carry

        lax.fori_loop(0, TILE // 64, scaled, 0, unroll=4)
        rows = pl.ds(t * TILE, TILE)
        copies.append(pltpu.make_async_copy(buffer.at[rows], out_hbm.at[rows], out_sem.at[t]))
        copies[-1].start()
    for copy in copies:
        copy.wait()
    scale_out.wait()


def shards(master_flat):
    flat = pltpu.with_memory_space_constraint(master_flat.reshape(ROWS * Z, HEADS_WIDTH), pltpu.HBM)
    gathered = pl.pallas_call(
        gather_kernel,
        name="gather",
        out_shape=jax.ShapeDtypeStruct((D, HEADS_WIDTH), jnp.bfloat16),
        in_specs=[pl.BlockSpec(memory_space=pltpu.HBM)],
        out_specs=pl.BlockSpec(memory_space=pltpu.VMEM),
        scratch_shapes=[
            pltpu.VMEM((ROWS * Z, HEADS_WIDTH), jnp.float32),
            pltpu.VMEM((Z, ROWS, HEADS_WIDTH), jnp.bfloat16),
            pltpu.SemaphoreType.DMA,
            pltpu.SemaphoreType.REGULAR((Z,)),
            pltpu.SemaphoreType.REGULAR,
            pltpu.SemaphoreType.DMA,
            pltpu.SemaphoreType.DMA((Z,)),
            pltpu.SemaphoreType.DMA,
            pltpu.SemaphoreType.DMA((X * Y,)),
            pltpu.SemaphoreType.DMA((X * Y,)),
            pltpu.SemaphoreType.DMA((X * Y,)),
            pltpu.SemaphoreType.DMA,
            pltpu.SemaphoreType.DMA,
        ],
        compiler_params=pltpu.CompilerParams(collective_id=0, has_side_effects=True, vmem_limit_bytes=16 * 1024 * 1024),
    )(flat)
    weight, scale = pl.pallas_call(
        scale_kernel,
        name="scale",
        out_shape=(jax.ShapeDtypeStruct((D, HEADS_WIDTH), jnp.bfloat16), jax.ShapeDtypeStruct((1, HEADS_WIDTH), jnp.float32)),
        in_specs=[pl.BlockSpec(memory_space=pltpu.VMEM)],
        out_specs=(pl.BlockSpec(memory_space=pl.ANY), pl.BlockSpec(memory_space=pl.ANY)),
        scratch_shapes=[
            pltpu.VMEM((D, HEADS_WIDTH), jnp.bfloat16),
            pltpu.VMEM((1, HEADS_WIDTH), jnp.float32),
            pltpu.SemaphoreType.DMA((D // TILE,)),
            pltpu.SemaphoreType.DMA,
        ],
        compiler_params=pltpu.CompilerParams(vmem_limit_bytes=16 * 1024 * 1024),
    )(gathered)
    return weight.reshape(1, D, HEADS_WIDTH), scale


def solution(mesh):
    return jax.shard_map(shards, mesh=mesh, in_specs=(P(("gx", "ta")),), out_specs=(P(None, None, "ta"), P(None, "ta")), check_vma=False)
```

```python
import functools

import jax
import jax.numpy as jnp
from jax import lax
from jax.experimental import pallas as pl
from jax.experimental.pallas import tpu as pltpu
from jax.sharding import PartitionSpec as P

D = 8192
HEADS_WIDTH = 128
X, Y, Z = 4, 8, 8
ROWS = 16
HALF = Z * ROWS
A_END, LATE = 2, 4
MESH = pl.DeviceIdType.MESH


def rank(at, size):
    return jnp.where(at * 2 <= size, jnp.maximum(2 * at - 1, 0), 2 * (size - at))


def order_of(step, size):
    return lax.rem(jnp.where(step % 2 == 1, (step + 1) // 2, size - step // 2), size)


def gather_kernel(x_hbm, out_ref, scale_ref, stage, rounded, load_sem, entered_z, entered, swap_send, swap_recv, send_sem, a_recv, b_recv, late_recv, core_send, core_recv, core_late):
    gx, z = lax.axis_index("gx"), lax.axis_index("ta")
    core, chip = lax.rem(gx, 2), gx // 2
    x, y = chip // Y, lax.rem(chip, Y)
    x_rank, y_rank = rank(x, X), rank(y, Y)

    load = pltpu.make_async_copy(x_hbm, stage, load_sem)
    load.start()

    barrier = pltpu.get_barrier_semaphore()

    def device(xt, yt, zt, ct):
        return ((xt * Y + yt) * 2 + ct, zt)

    def signal(semaphore, to):
        pl.semaphore_signal(semaphore, inc=1, device_id=to, device_id_type=MESH)

    def around(size, at, then):
        for d in range(1, size):
            then(lax.rem(at + d, size))

    def greet(later, to):
        @pl.when(later)
        def _():
            signal(barrier, to)

    greet(core == 1, device(x, y, z, 1 - core))
    around(Z, z, lambda zt: greet(zt > z, device(x, y, zt, core)))
    around(Y, y, lambda yt: greet(rank(yt, Y) > y_rank, device(x, yt, z, core)))
    around(X, x, lambda xt: greet(rank(xt, X) > x_rank, device(xt, y, z, core)))

    def rows_of(xt, yt, ct, offset, count):
        start = ((xt * Y + yt) * 2 + ct) * HALF + offset
        return pl.ds(pl.multiple_of(start, ROWS), count)

    def wait_for(semaphore, count):
        @pl.when(count > 0)
        def _():
            pl.semaphore_wait(semaphore, count)

    wait_for(barrier, (1 - core) + z + y_rank + x_rank)

    def answer(earlier, semaphore, to):
        @pl.when(earlier)
        def _():
            signal(semaphore, to)

    around(Z, z, lambda zt: answer(zt < z, entered_z.at[z], device(x, y, zt, core)))
    around(Y, y, lambda yt: answer(rank(yt, Y) < y_rank, entered, device(x, yt, z, core)))
    around(X, x, lambda xt: answer(rank(xt, X) < x_rank, entered, device(xt, y, z, core)))
    answer(core == 0, entered, device(x, y, z, 1 - core))

    load.wait()
    for k in range(Z):
        rounded[k] = stage[pl.ds(k, ROWS, stride=Z), :].astype(jnp.bfloat16)
    here = rows_of(x, y, core, z * ROWS, ROWS)
    out_ref[here, :] = rounded[z]

    def remote(src, dst, send, recv, to):
        return pltpu.make_async_remote_copy(src_ref=src, dst_ref=dst, send_sem=send, recv_sem=recv, device_id=to, device_id_type=MESH)

    def swap(zt):
        @pl.when(zt > z)
        def _():
            pl.semaphore_wait(entered_z.at[zt], 1)

        remote(rounded.at[zt], out_ref.at[here], swap_send, swap_recv.at[z], device(x, y, zt, core)).start()

    def swap_soon(zt, carry):
        @pl.when((zt != z) & ((zt < z) | (zt < LATE)))
        def _():
            swap(zt)

        return carry

    def swap_rest(zt, carry):
        @pl.when(zt > z)
        def _():
            swap(zt)

        return carry

    def waiter(ref, sem):
        pltpu.make_async_copy(ref, ref, sem).wait()

    def swapped(zt, carry):
        @pl.when(zt != z)
        def _():
            waiter(rounded.at[zt], swap_recv.at[zt])

        return carry

    def along_y(ref, recv):
        for d in (4, 3, 5, 2, 6, 1, 7):
            remote(ref, ref, send_sem, recv, device(x, lax.rem(y + d, Y), z, core)).start()

    def along_x(ref, recv):
        for d in (2, 1, 3):
            remote(ref, ref, send_sem, recv, device(lax.rem(x + d, X), y, z, core)).start()

    def across(ref, recv):
        remote(ref, ref, core_send, recv, device(x, y, z, 1 - core)).start()

    def part_a(xt, yt):
        return out_ref.at[rows_of(xt, yt, core, 0, A_END * ROWS)]

    def part_b(xt, yt):
        return out_ref.at[rows_of(xt, yt, core, A_END * ROWS, (LATE - A_END) * ROWS)]

    def part_late(xt, yt):
        return out_ref.at[rows_of(xt, yt, core, LATE * ROWS, (Z - LATE) * ROWS)]

    def early(xt, yt):
        return out_ref.at[rows_of(xt, yt, core, 0, LATE * ROWS)]

    lax.fori_loop(0, Z, swap_soon, 0)
    lax.fori_loop(0, A_END, swapped, 0)
    wait_for(entered, (Y - 1 - y_rank) + (X - 1 - x_rank) + core)
    along_x(part_a(x, y), a_recv.at[chip])
    along_y(part_a(x, y), a_recv.at[chip])
    lax.fori_loop(LATE, Z, swap_rest, 0)
    lax.fori_loop(A_END, LATE, swapped, 0)
    along_y(part_b(x, y), b_recv.at[chip])
    along_x(part_b(x, y), b_recv.at[chip])
    across(early(x, y), core_recv)
    lax.fori_loop(LATE, Z, swapped, 0)
    along_y(part_late(x, y), late_recv.at[chip])
    along_x(part_late(x, y), late_recv.at[chip])
    across(part_late(x, y), core_late)

    def forward(part, recv, step, over_x):
        xt, yt = (order_of(step, X), y) if over_x else (x, order_of(step, Y))

        @pl.when((xt != x) | (yt != y))
        def _():
            ref, sem = part(xt, yt), recv.at[xt * Y + yt]
            waiter(ref, sem)
            (along_y if over_x else along_x)(ref, sem)

        return 0

    from_x = lambda step, carry: forward(part_a, a_recv, step, True)
    from_y = lambda step, carry: forward(part_b, b_recv, step, False)
    late_from_y = lambda step, carry: forward(part_late, late_recv, step, False)
    lax.fori_loop(0, X, from_x, 0)
    lax.fori_loop(0, Y, from_y, 0)
    lax.fori_loop(0, Y, late_from_y, 0)

    def arrival(step, carry):
        xt, yt = order_of(step // 8, X), order_of(lax.rem(step, 8), Y)
        source = xt * Y + yt

        @pl.when(source != chip)
        def _():
            @pl.when(yt != y)
            def _():
                waiter(part_a(xt, yt), a_recv.at[source])

            @pl.when(xt != x)
            def _():
                waiter(part_b(xt, yt), b_recv.at[source])

            across(early(xt, yt), core_recv)

        return carry

    def late_arrival(step, carry):
        xt, yt = order_of(step // 8, X), order_of(lax.rem(step, 8), Y)
        source = xt * Y + yt

        @pl.when(source != chip)
        def _():
            @pl.when(xt != x)
            def _():
                waiter(part_late(xt, yt), late_recv.at[source])

            across(part_late(xt, yt), core_late)

        return carry

    lax.fori_loop(0, X * Y, arrival, 0)
    lax.fori_loop(0, X * Y, late_arrival, 0)

    def largest(ct, offset, count, best):
        def step(p, best):
            block = jnp.abs(out_ref[pl.ds(pl.multiple_of((p * 2 + ct) * HALF + offset, ROWS), count), :])
            return jnp.maximum(best, jnp.max(block.reshape(count // 32, 32, HEADS_WIDTH), axis=0))

        return lax.fori_loop(0, X * Y, step, best, unroll=4)

    best = largest(core, 0, HALF, jnp.zeros((32, HEADS_WIDTH), jnp.bfloat16))
    waiter(out_ref.at[pl.ds(0, X * Y * LATE * ROWS)], core_recv)
    best = largest(1 - core, 0, LATE * ROWS, best)
    waiter(out_ref.at[pl.ds(0, X * Y * (Z - LATE) * ROWS)], core_late)
    best = largest(1 - core, LATE * ROWS, (Z - LATE) * ROWS, best)
    scale_ref[...] = jnp.max(best.astype(jnp.float32), axis=0, keepdims=True)
    waiter(out_ref.at[pl.ds(0, (Z - 1) * ROWS)], swap_send)
    a_rows, b_rows = A_END * ROWS, (Z - A_END) * ROWS
    sent = a_rows * ((X - 1) + X * (Y - 1)) + b_rows * ((Y - 1) + Y * (X - 1))
    waiter(out_ref.at[pl.ds(0, sent)], send_sem)
    waiter(out_ref.at[pl.ds(0, D // 2)], core_send)


TILES = (512, 512, 1024, 1024, 1024, 1024, 1024, 1024, 512, 512)


def scale_kernel(w_ref, scale_ref, out_hbm, scale_hbm, buffer, out_sem, scale_sem):
    scale_out = pltpu.make_async_copy(scale_ref, scale_hbm, scale_sem)
    scale_out.start()
    inverse = jnp.broadcast_to(1.0 / scale_ref[...], (64, HEADS_WIDTH))
    copies, start = [], 0
    for t, tile in enumerate(TILES):
        def scaled(i, carry, start=start):
            rows = pl.ds(pl.multiple_of(start + i * 64, 64), 64)
            buffer[rows, :] = (w_ref[rows, :].astype(jnp.float32) * inverse).astype(jnp.bfloat16)
            return carry

        lax.fori_loop(0, tile // 64, scaled, 0, unroll=4)
        rows = pl.ds(start, tile)
        copies.append(pltpu.make_async_copy(buffer.at[rows], out_hbm.at[rows], out_sem.at[t]))
        copies[-1].start()
        start += tile
    for copy in copies:
        copy.wait()
    scale_out.wait()


def shards(master_flat):
    flat = pltpu.with_memory_space_constraint(master_flat.reshape(ROWS * Z, HEADS_WIDTH), pltpu.HBM)
    gathered, largest = pl.pallas_call(
        gather_kernel,
        name="gather",
        out_shape=(jax.ShapeDtypeStruct((D, HEADS_WIDTH), jnp.bfloat16), jax.ShapeDtypeStruct((1, HEADS_WIDTH), jnp.float32)),
        in_specs=[pl.BlockSpec(memory_space=pltpu.HBM)],
        out_specs=(pl.BlockSpec(memory_space=pltpu.VMEM), pl.BlockSpec(memory_space=pltpu.VMEM)),
        scratch_shapes=[
            pltpu.VMEM((ROWS * Z, HEADS_WIDTH), jnp.float32),
            pltpu.VMEM((Z, ROWS, HEADS_WIDTH), jnp.bfloat16),
            pltpu.SemaphoreType.DMA,
            pltpu.SemaphoreType.REGULAR((Z,)),
            pltpu.SemaphoreType.REGULAR,
            pltpu.SemaphoreType.DMA,
            pltpu.SemaphoreType.DMA((Z,)),
            pltpu.SemaphoreType.DMA,
            pltpu.SemaphoreType.DMA((X * Y,)),
            pltpu.SemaphoreType.DMA((X * Y,)),
            pltpu.SemaphoreType.DMA((X * Y,)),
            pltpu.SemaphoreType.DMA,
            pltpu.SemaphoreType.DMA,
            pltpu.SemaphoreType.DMA,
        ],
        compiler_params=pltpu.CompilerParams(collective_id=0, has_side_effects=True, vmem_limit_bytes=16 * 1024 * 1024),
    )(flat)
    weight, scale = pl.pallas_call(
        scale_kernel,
        name="scale",
        out_shape=(jax.ShapeDtypeStruct((D, HEADS_WIDTH), jnp.bfloat16), jax.ShapeDtypeStruct((1, HEADS_WIDTH), jnp.float32)),
        in_specs=[pl.BlockSpec(memory_space=pltpu.VMEM), pl.BlockSpec(memory_space=pltpu.VMEM)],
        out_specs=(pl.BlockSpec(memory_space=pl.ANY), pl.BlockSpec(memory_space=pl.ANY)),
        scratch_shapes=[
            pltpu.VMEM((D, HEADS_WIDTH), jnp.bfloat16),
            pltpu.SemaphoreType.DMA((len(TILES),)),
            pltpu.SemaphoreType.DMA,
        ],
        compiler_params=pltpu.CompilerParams(vmem_limit_bytes=16 * 1024 * 1024),
    )(gathered, largest)
    return weight.reshape(1, D, HEADS_WIDTH), scale


def solution(mesh):
    return jax.shard_map(shards, mesh=mesh, in_specs=(P(("gx", "ta")),), out_specs=(P(None, None, "ta"), P(None, "ta")), check_vma=False)
```

```python
import functools

import jax
import jax.numpy as jnp
from jax import lax
from jax.experimental import pallas as pl
from jax.experimental.pallas import tpu as pltpu
from jax.sharding import PartitionSpec as P

D = 8192
HEADS_WIDTH = 128
X, Y, Z = 4, 8, 8
ROWS = 16
HALF = Z * ROWS
A_END, LATE = 2, 4
MESH = pl.DeviceIdType.MESH


def rank(at, size):
    return jnp.where(at * 2 <= size, jnp.maximum(2 * at - 1, 0), 2 * (size - at))


def order_of(step, size):
    return lax.rem(jnp.where(step % 2 == 1, (step + 1) // 2, size - step // 2), size)


def gather_kernel(x_hbm, out_ref, scale_ref, stage, rounded, load_sem, entered_z, entered, swap_send, swap_recv, send_sem, a_recv, b_recv, late_recv, core_send, core_recv, core_late):
    gx, z = lax.axis_index("gx"), lax.axis_index("ta")
    core, chip = lax.rem(gx, 2), gx // 2
    x, y = chip // Y, lax.rem(chip, Y)
    x_rank, y_rank = rank(x, X), rank(y, Y)

    load = pltpu.make_async_copy(x_hbm, stage, load_sem)
    load.start()

    barrier = pltpu.get_barrier_semaphore()

    def device(xt, yt, zt, ct):
        return ((xt * Y + yt) * 2 + ct, zt)

    def signal(semaphore, to):
        pl.semaphore_signal(semaphore, inc=1, device_id=to, device_id_type=MESH)

    def around(size, at, then):
        for d in range(1, size):
            then(lax.rem(at + d, size))

    def greet(later, to):
        @pl.when(later)
        def _():
            signal(barrier, to)

    greet(core == 1, device(x, y, z, 1 - core))
    around(Z, z, lambda zt: greet(zt > z, device(x, y, zt, core)))
    around(Y, y, lambda yt: greet(rank(yt, Y) > y_rank, device(x, yt, z, core)))
    around(X, x, lambda xt: greet(rank(xt, X) > x_rank, device(xt, y, z, core)))

    def rows_of(xt, yt, ct, offset, count):
        start = ((xt * Y + yt) * 2 + ct) * HALF + offset
        return pl.ds(pl.multiple_of(start, ROWS), count)

    def wait_for(semaphore, count):
        @pl.when(count > 0)
        def _():
            pl.semaphore_wait(semaphore, count)

    wait_for(barrier, (1 - core) + z + y_rank + x_rank)

    def answer(earlier, semaphore, to):
        @pl.when(earlier)
        def _():
            signal(semaphore, to)

    around(Z, z, lambda zt: answer(zt < z, entered_z.at[z], device(x, y, zt, core)))
    around(Y, y, lambda yt: answer(rank(yt, Y) < y_rank, entered, device(x, yt, z, core)))
    around(X, x, lambda xt: answer(rank(xt, X) < x_rank, entered, device(xt, y, z, core)))
    answer(core == 0, entered, device(x, y, z, 1 - core))

    load.wait()
    for k in range(Z):
        rounded[k] = stage[pl.ds(k, ROWS, stride=Z), :].astype(jnp.bfloat16)
    here = rows_of(x, y, core, z * ROWS, ROWS)
    out_ref[here, :] = rounded[z]

    def remote(src, dst, send, recv, to):
        return pltpu.make_async_remote_copy(src_ref=src, dst_ref=dst, send_sem=send, recv_sem=recv, device_id=to, device_id_type=MESH)

    def swap(zt):
        @pl.when(zt > z)
        def _():
            pl.semaphore_wait(entered_z.at[zt], 1)

        remote(rounded.at[zt], out_ref.at[here], swap_send, swap_recv.at[z], device(x, y, zt, core)).start()

    def swap_soon(zt, carry):
        @pl.when((zt != z) & ((zt < z) | (zt < LATE)))
        def _():
            swap(zt)

        return carry

    def swap_rest(zt, carry):
        @pl.when(zt > z)
        def _():
            swap(zt)

        return carry

    def waiter(ref, sem):
        pltpu.make_async_copy(ref, ref, sem).wait()

    def swapped(zt, carry):
        @pl.when(zt != z)
        def _():
            waiter(rounded.at[zt], swap_recv.at[zt])

        return carry

    def along_y(ref, recv):
        for d in (1, 7, 2, 6, 3, 5, 4):
            remote(ref, ref, send_sem, recv, device(x, lax.rem(y + d, Y), z, core)).start()

    def along_x(ref, recv):
        for d in (2, 1, 3):
            remote(ref, ref, send_sem, recv, device(lax.rem(x + d, X), y, z, core)).start()

    def across(ref, recv):
        remote(ref, ref, core_send, recv, device(x, y, z, 1 - core)).start()

    def part_a(xt, yt):
        return out_ref.at[rows_of(xt, yt, core, 0, A_END * ROWS)]

    def part_b(xt, yt):
        return out_ref.at[rows_of(xt, yt, core, A_END * ROWS, (LATE - A_END) * ROWS)]

    def part_late(xt, yt):
        return out_ref.at[rows_of(xt, yt, core, LATE * ROWS, (Z - LATE) * ROWS)]

    def early(xt, yt):
        return out_ref.at[rows_of(xt, yt, core, 0, LATE * ROWS)]

    def own_a():
        lax.fori_loop(0, A_END, swapped, 0)
        along_x(part_a(x, y), a_recv.at[chip])
        along_y(part_a(x, y), a_recv.at[chip])

    def own_b():
        lax.fori_loop(A_END, LATE, swapped, 0)
        along_y(part_b(x, y), b_recv.at[chip])
        along_x(part_b(x, y), b_recv.at[chip])
        across(early(x, y), core_recv)

    def own_late():
        lax.fori_loop(LATE, Z, swapped, 0)
        along_y(part_late(x, y), late_recv.at[chip])
        along_x(part_late(x, y), late_recv.at[chip])
        across(part_late(x, y), core_late)

    def forward(part, recv, step, over_x):
        xt, yt = (order_of(step, X), y) if over_x else (x, order_of(step, Y))

        @pl.when((xt != x) | (yt != y))
        def _():
            ref, sem = part(xt, yt), recv.at[xt * Y + yt]
            waiter(ref, sem)
            (along_y if over_x else along_x)(ref, sem)

        return 0

    from_x = lambda step, carry: forward(part_a, a_recv, step, True)
    from_y = lambda step, carry: forward(part_b, b_recv, step, False)
    late_from_y = lambda step, carry: forward(part_late, late_recv, step, False)
    def loop(start, end, body):
        lax.fori_loop(start, end, body, 0)

    loop(0, Z, swap_soon)

    @pl.when(z < LATE)
    def _():
        wait_for(entered, (Y - 1 - y_rank) + (X - 1 - x_rank) + core)
        own_a()
        loop(LATE, Z, swap_rest)
        own_b()
        own_late()
        loop(0, 3, from_x)
        loop(0, Y, from_y)
        loop(3, X, from_x)
        loop(0, Y, late_from_y)

    @pl.when(z >= LATE)
    def _():
        loop(LATE, Z, swap_rest)
        wait_for(entered, (Y - 1 - y_rank) + (X - 1 - x_rank) + core)
        own_late()
        own_a()
        own_b()
        loop(0, X, from_x)
        loop(0, Y, late_from_y)
        loop(0, Y, from_y)

    def arrival(step, carry):
        xt, yt = order_of(step // 8, X), order_of(lax.rem(step, 8), Y)
        source = xt * Y + yt

        @pl.when(source != chip)
        def _():
            @pl.when(yt != y)
            def _():
                waiter(part_a(xt, yt), a_recv.at[source])

            @pl.when(xt != x)
            def _():
                waiter(part_b(xt, yt), b_recv.at[source])

            across(early(xt, yt), core_recv)

        return carry

    def late_arrival(step, carry):
        xt, yt = order_of(step // 8, X), order_of(lax.rem(step, 8), Y)
        source = xt * Y + yt

        @pl.when(source != chip)
        def _():
            @pl.when(xt != x)
            def _():
                waiter(part_late(xt, yt), late_recv.at[source])

            across(part_late(xt, yt), core_late)

        return carry

    lax.fori_loop(0, X * Y, arrival, 0)
    lax.fori_loop(0, X * Y, late_arrival, 0)

    def largest(ct, offset, count, best):
        def step(p, best):
            block = jnp.abs(out_ref[pl.ds(pl.multiple_of((p * 2 + ct) * HALF + offset, ROWS), count), :])
            return jnp.maximum(best, jnp.max(block.reshape(count // 32, 32, HEADS_WIDTH), axis=0))

        return lax.fori_loop(0, X * Y, step, best, unroll=4)

    best = largest(core, 0, HALF, jnp.zeros((32, HEADS_WIDTH), jnp.bfloat16))
    waiter(out_ref.at[pl.ds(0, X * Y * LATE * ROWS)], core_recv)
    best = largest(1 - core, 0, LATE * ROWS, best)
    waiter(out_ref.at[pl.ds(0, X * Y * (Z - LATE) * ROWS)], core_late)
    best = largest(1 - core, LATE * ROWS, (Z - LATE) * ROWS, best)
    scale_ref[...] = jnp.max(best.astype(jnp.float32), axis=0, keepdims=True)
    waiter(out_ref.at[pl.ds(0, (Z - 1) * ROWS)], swap_send)
    a_rows, b_rows = A_END * ROWS, (Z - A_END) * ROWS
    sent = a_rows * ((X - 1) + X * (Y - 1)) + b_rows * ((Y - 1) + Y * (X - 1))
    waiter(out_ref.at[pl.ds(0, sent)], send_sem)
    waiter(out_ref.at[pl.ds(0, D // 2)], core_send)


TILES = (512, 512, 1024, 1024, 1024, 1024, 1024, 1024, 512, 512)


def scale_kernel(w_ref, scale_ref, out_hbm, scale_hbm, buffer, out_sem, scale_sem):
    scale_out = pltpu.make_async_copy(scale_ref, scale_hbm, scale_sem)
    scale_out.start()
    inverse = jnp.broadcast_to(1.0 / scale_ref[...], (64, HEADS_WIDTH))
    copies, start = [], 0
    for t, tile in enumerate(TILES):
        def scaled(i, carry, start=start):
            rows = pl.ds(pl.multiple_of(start + i * 64, 64), 64)
            buffer[rows, :] = (w_ref[rows, :].astype(jnp.float32) * inverse).astype(jnp.bfloat16)
            return carry

        lax.fori_loop(0, tile // 64, scaled, 0, unroll=4)
        rows = pl.ds(start, tile)
        copies.append(pltpu.make_async_copy(buffer.at[rows], out_hbm.at[rows], out_sem.at[t]))
        copies[-1].start()
        start += tile
    for copy in copies:
        copy.wait()
    scale_out.wait()


def shards(master_flat):
    flat = pltpu.with_memory_space_constraint(master_flat.reshape(ROWS * Z, HEADS_WIDTH), pltpu.HBM)
    gathered, largest = pl.pallas_call(
        gather_kernel,
        name="gather",
        out_shape=(jax.ShapeDtypeStruct((D, HEADS_WIDTH), jnp.bfloat16), jax.ShapeDtypeStruct((1, HEADS_WIDTH), jnp.float32)),
        in_specs=[pl.BlockSpec(memory_space=pltpu.HBM)],
        out_specs=(pl.BlockSpec(memory_space=pltpu.VMEM), pl.BlockSpec(memory_space=pltpu.VMEM)),
        scratch_shapes=[
            pltpu.VMEM((ROWS * Z, HEADS_WIDTH), jnp.float32),
            pltpu.VMEM((Z, ROWS, HEADS_WIDTH), jnp.bfloat16),
            pltpu.SemaphoreType.DMA,
            pltpu.SemaphoreType.REGULAR((Z,)),
            pltpu.SemaphoreType.REGULAR,
            pltpu.SemaphoreType.DMA,
            pltpu.SemaphoreType.DMA((Z,)),
            pltpu.SemaphoreType.DMA,
            pltpu.SemaphoreType.DMA((X * Y,)),
            pltpu.SemaphoreType.DMA((X * Y,)),
            pltpu.SemaphoreType.DMA((X * Y,)),
            pltpu.SemaphoreType.DMA,
            pltpu.SemaphoreType.DMA,
            pltpu.SemaphoreType.DMA,
        ],
        compiler_params=pltpu.CompilerParams(collective_id=0, has_side_effects=True, vmem_limit_bytes=16 * 1024 * 1024),
    )(flat)
    weight, scale = pl.pallas_call(
        scale_kernel,
        name="scale",
        out_shape=(jax.ShapeDtypeStruct((D, HEADS_WIDTH), jnp.bfloat16), jax.ShapeDtypeStruct((1, HEADS_WIDTH), jnp.float32)),
        in_specs=[pl.BlockSpec(memory_space=pltpu.VMEM), pl.BlockSpec(memory_space=pltpu.VMEM)],
        out_specs=(pl.BlockSpec(memory_space=pl.ANY), pl.BlockSpec(memory_space=pl.ANY)),
        scratch_shapes=[
            pltpu.VMEM((D, HEADS_WIDTH), jnp.bfloat16),
            pltpu.SemaphoreType.DMA((len(TILES),)),
            pltpu.SemaphoreType.DMA,
        ],
        compiler_params=pltpu.CompilerParams(vmem_limit_bytes=16 * 1024 * 1024),
    )(gathered, largest)
    return weight.reshape(1, D, HEADS_WIDTH), scale


def solution(mesh):
    return jax.shard_map(shards, mesh=mesh, in_specs=(P(("gx", "ta")),), out_specs=(P(None, None, "ta"), P(None, "ta")), check_vma=False)
```

```python
import functools

import jax
import jax.numpy as jnp
from jax import lax
from jax.experimental import pallas as pl
from jax.experimental.pallas import tpu as pltpu
from jax.sharding import PartitionSpec as P

D = 8192
HEADS_WIDTH = 128
X, Y, Z = 4, 8, 8
ROWS = 16
HALF = Z * ROWS
A_END, LATE = 2, 4
MESH = pl.DeviceIdType.MESH


def rank(at, size):
    return jnp.where(at * 2 <= size, jnp.maximum(2 * at - 1, 0), 2 * (size - at))


def order_of(step, size):
    return lax.rem(jnp.where(step % 2 == 1, (step + 1) // 2, size - step // 2), size)


def gather_kernel(x_hbm, out_ref, scale_ref, stage, rounded, load_sem, entered_z, entered, swap_send, swap_recv, send_sem, a_recv, b_recv, late_recv, core_send, core_recv, core_late):
    gx, z = lax.axis_index("gx"), lax.axis_index("ta")
    core, chip = lax.rem(gx, 2), gx // 2
    x, y = chip // Y, lax.rem(chip, Y)
    x_rank, y_rank = rank(x, X), rank(y, Y)

    load = pltpu.make_async_copy(x_hbm, stage, load_sem)
    load.start()

    barrier = pltpu.get_barrier_semaphore()

    def device(xt, yt, zt, ct):
        return ((xt * Y + yt) * 2 + ct, zt)

    def signal(semaphore, to):
        pl.semaphore_signal(semaphore, inc=1, device_id=to, device_id_type=MESH)

    def around(size, at, then):
        for d in range(1, size):
            then(lax.rem(at + d, size))

    def greet(later, to):
        @pl.when(later)
        def _():
            signal(barrier, to)

    greet(core == 1, device(x, y, z, 1 - core))
    around(Z, z, lambda zt: greet(zt > z, device(x, y, zt, core)))
    around(Y, y, lambda yt: greet(rank(yt, Y) > y_rank, device(x, yt, z, core)))
    around(X, x, lambda xt: greet(rank(xt, X) > x_rank, device(xt, y, z, core)))

    def rows_of(xt, yt, ct, offset, count):
        start = ((xt * Y + yt) * 2 + ct) * HALF + offset
        return pl.ds(pl.multiple_of(start, ROWS), count)

    def wait_for(semaphore, count):
        @pl.when(count > 0)
        def _():
            pl.semaphore_wait(semaphore, count)

    wait_for(barrier, (1 - core) + z + y_rank + x_rank)

    def answer(earlier, semaphore, to):
        @pl.when(earlier)
        def _():
            signal(semaphore, to)

    around(Z, z, lambda zt: answer(zt < z, entered_z.at[z], device(x, y, zt, core)))
    around(Y, y, lambda yt: answer(rank(yt, Y) < y_rank, entered, device(x, yt, z, core)))
    around(X, x, lambda xt: answer(rank(xt, X) < x_rank, entered, device(xt, y, z, core)))
    answer(core == 0, entered, device(x, y, z, 1 - core))

    load.wait()
    for k in range(Z):
        rounded[k] = stage[pl.ds(k, ROWS, stride=Z), :].astype(jnp.bfloat16)
    here = rows_of(x, y, core, z * ROWS, ROWS)
    out_ref[here, :] = rounded[z]

    def remote(src, dst, send, recv, to):
        return pltpu.make_async_remote_copy(src_ref=src, dst_ref=dst, send_sem=send, recv_sem=recv, device_id=to, device_id_type=MESH)

    def swap(zt):
        @pl.when(zt > z)
        def _():
            pl.semaphore_wait(entered_z.at[zt], 1)

        remote(rounded.at[zt], out_ref.at[here], swap_send, swap_recv.at[z], device(x, y, zt, core)).start()

    def swap_soon(zt, carry):
        @pl.when((zt != z) & ((zt < z) | (zt < LATE)))
        def _():
            swap(zt)

        return carry

    def swap_rest(zt, carry):
        @pl.when(zt > z)
        def _():
            swap(zt)

        return carry

    def waiter(ref, sem):
        pltpu.make_async_copy(ref, ref, sem).wait()

    def swapped(zt, carry):
        @pl.when(zt != z)
        def _():
            waiter(rounded.at[zt], swap_recv.at[zt])

        return carry

    def along_y(ref, recv):
        for d in (1, 7, 2, 6, 3, 5, 4):
            remote(ref, ref, send_sem, recv, device(x, lax.rem(y + d, Y), z, core)).start()

    def along_x(ref, recv):
        for d in (1, 3, 2):
            remote(ref, ref, send_sem, recv, device(lax.rem(x + d, X), y, z, core)).start()

    def across(ref, recv):
        remote(ref, ref, core_send, recv, device(x, y, z, 1 - core)).start()

    def part_a(xt, yt):
        return out_ref.at[rows_of(xt, yt, core, 0, A_END * ROWS)]

    def part_b(xt, yt):
        return out_ref.at[rows_of(xt, yt, core, A_END * ROWS, (LATE - A_END) * ROWS)]

    def part_late(xt, yt):
        return out_ref.at[rows_of(xt, yt, core, LATE * ROWS, (Z - LATE) * ROWS)]

    def early(xt, yt):
        return out_ref.at[rows_of(xt, yt, core, 0, LATE * ROWS)]

    def own_a():
        lax.fori_loop(0, A_END, swapped, 0)
        along_x(part_a(x, y), a_recv.at[chip])
        along_y(part_a(x, y), a_recv.at[chip])

    def own_b():
        lax.fori_loop(A_END, LATE, swapped, 0)
        along_y(part_b(x, y), b_recv.at[chip])
        along_x(part_b(x, y), b_recv.at[chip])
        across(early(x, y), core_recv)

    def own_late():
        lax.fori_loop(LATE, Z, swapped, 0)
        along_y(part_late(x, y), late_recv.at[chip])
        along_x(part_late(x, y), late_recv.at[chip])
        across(part_late(x, y), core_late)

    def forward(part, recv, step, over_x):
        xt, yt = (order_of(step, X), y) if over_x else (x, order_of(step, Y))

        @pl.when((xt != x) | (yt != y))
        def _():
            ref, sem = part(xt, yt), recv.at[xt * Y + yt]
            waiter(ref, sem)
            (along_y if over_x else along_x)(ref, sem)

        return 0

    from_x = lambda step, carry: forward(part_a, a_recv, step, True)
    from_y = lambda step, carry: forward(part_b, b_recv, step, False)
    late_from_y = lambda step, carry: forward(part_late, late_recv, step, False)
    def loop(start, end, body):
        lax.fori_loop(start, end, body, 0)

    loop(0, Z, swap_soon)

    @pl.when(z < LATE)
    def _():
        wait_for(entered, (Y - 1 - y_rank) + (X - 1 - x_rank) + core)
        own_a()
        loop(LATE, Z, swap_rest)
        own_b()
        own_late()
        loop(0, 3, from_x)
        loop(0, Y, from_y)
        loop(3, X, from_x)
        loop(0, Y, late_from_y)

    @pl.when(z >= LATE)
    def _():
        loop(LATE, Z, swap_rest)
        wait_for(entered, (Y - 1 - y_rank) + (X - 1 - x_rank) + core)
        own_late()
        own_a()
        own_b()
        loop(0, X, from_x)
        loop(0, Y, late_from_y)
        loop(0, Y, from_y)

    def arrival(step, carry):
        xt, yt = order_of(step // 8, X), order_of(lax.rem(step, 8), Y)
        source = xt * Y + yt

        @pl.when(source != chip)
        def _():
            @pl.when(yt != y)
            def _():
                waiter(part_a(xt, yt), a_recv.at[source])

            @pl.when(xt != x)
            def _():
                waiter(part_b(xt, yt), b_recv.at[source])

            across(early(xt, yt), core_recv)

        return carry

    def late_arrival(step, carry):
        xt, yt = order_of(step // 8, X), order_of(lax.rem(step, 8), Y)
        source = xt * Y + yt

        @pl.when(source != chip)
        def _():
            @pl.when(xt != x)
            def _():
                waiter(part_late(xt, yt), late_recv.at[source])

            across(part_late(xt, yt), core_late)

        return carry

    lax.fori_loop(0, X * Y, arrival, 0)
    lax.fori_loop(0, X * Y, late_arrival, 0)

    def largest(ct, offset, count, best):
        def step(p, best):
            block = jnp.abs(out_ref[pl.ds(pl.multiple_of((p * 2 + ct) * HALF + offset, ROWS), count), :])
            return jnp.maximum(best, jnp.max(block.reshape(count // 32, 32, HEADS_WIDTH), axis=0))

        return lax.fori_loop(0, X * Y, step, best, unroll=4)

    best = largest(core, 0, HALF, jnp.zeros((32, HEADS_WIDTH), jnp.bfloat16))
    waiter(out_ref.at[pl.ds(0, X * Y * LATE * ROWS)], core_recv)
    best = largest(1 - core, 0, LATE * ROWS, best)
    waiter(out_ref.at[pl.ds(0, X * Y * (Z - LATE) * ROWS)], core_late)
    best = largest(1 - core, LATE * ROWS, (Z - LATE) * ROWS, best)
    scale_ref[...] = jnp.max(best.astype(jnp.float32), axis=0, keepdims=True)
    waiter(out_ref.at[pl.ds(0, (Z - 1) * ROWS)], swap_send)
    a_rows, b_rows = A_END * ROWS, (Z - A_END) * ROWS
    sent = a_rows * ((X - 1) + X * (Y - 1)) + b_rows * ((Y - 1) + Y * (X - 1))
    waiter(out_ref.at[pl.ds(0, sent)], send_sem)
    waiter(out_ref.at[pl.ds(0, D // 2)], core_send)


TILES = (512, 512, 1024, 1024, 1024, 1024, 1024, 1024, 512, 512)


def scale_kernel(w_ref, scale_ref, out_hbm, scale_hbm, buffer, out_sem, scale_sem):
    scale_out = pltpu.make_async_copy(scale_ref, scale_hbm, scale_sem)
    scale_out.start()
    inverse = jnp.broadcast_to(1.0 / scale_ref[...], (64, HEADS_WIDTH))
    copies, start = [], 0
    for t, tile in enumerate(TILES):
        def scaled(i, carry, start=start):
            rows = pl.ds(pl.multiple_of(start + i * 64, 64), 64)
            buffer[rows, :] = (w_ref[rows, :].astype(jnp.float32) * inverse).astype(jnp.bfloat16)
            return carry

        lax.fori_loop(0, tile // 64, scaled, 0, unroll=8)
        rows = pl.ds(start, tile)
        copies.append(pltpu.make_async_copy(buffer.at[rows], out_hbm.at[rows], out_sem.at[t]))
        copies[-1].start()
        start += tile
    for copy in copies:
        copy.wait()
    scale_out.wait()


def shards(master_flat):
    flat = pltpu.with_memory_space_constraint(master_flat.reshape(ROWS * Z, HEADS_WIDTH), pltpu.HBM)
    gathered, largest = pl.pallas_call(
        gather_kernel,
        name="gather",
        out_shape=(jax.ShapeDtypeStruct((D, HEADS_WIDTH), jnp.bfloat16), jax.ShapeDtypeStruct((1, HEADS_WIDTH), jnp.float32)),
        in_specs=[pl.BlockSpec(memory_space=pltpu.HBM)],
        out_specs=(pl.BlockSpec(memory_space=pltpu.VMEM), pl.BlockSpec(memory_space=pltpu.VMEM)),
        scratch_shapes=[
            pltpu.VMEM((ROWS * Z, HEADS_WIDTH), jnp.float32),
            pltpu.VMEM((Z, ROWS, HEADS_WIDTH), jnp.bfloat16),
            pltpu.SemaphoreType.DMA,
            pltpu.SemaphoreType.REGULAR((Z,)),
            pltpu.SemaphoreType.REGULAR,
            pltpu.SemaphoreType.DMA,
            pltpu.SemaphoreType.DMA((Z,)),
            pltpu.SemaphoreType.DMA,
            pltpu.SemaphoreType.DMA((X * Y,)),
            pltpu.SemaphoreType.DMA((X * Y,)),
            pltpu.SemaphoreType.DMA((X * Y,)),
            pltpu.SemaphoreType.DMA,
            pltpu.SemaphoreType.DMA,
            pltpu.SemaphoreType.DMA,
        ],
        compiler_params=pltpu.CompilerParams(collective_id=0, has_side_effects=True, vmem_limit_bytes=16 * 1024 * 1024),
    )(flat)
    weight, scale = pl.pallas_call(
        scale_kernel,
        name="scale",
        out_shape=(jax.ShapeDtypeStruct((D, HEADS_WIDTH), jnp.bfloat16), jax.ShapeDtypeStruct((1, HEADS_WIDTH), jnp.float32)),
        in_specs=[pl.BlockSpec(memory_space=pltpu.VMEM), pl.BlockSpec(memory_space=pltpu.VMEM)],
        out_specs=(pl.BlockSpec(memory_space=pl.ANY), pl.BlockSpec(memory_space=pl.ANY)),
        scratch_shapes=[
            pltpu.VMEM((D, HEADS_WIDTH), jnp.bfloat16),
            pltpu.SemaphoreType.DMA((len(TILES),)),
            pltpu.SemaphoreType.DMA,
        ],
        compiler_params=pltpu.CompilerParams(vmem_limit_bytes=16 * 1024 * 1024),
    )(gathered, largest)
    return weight.reshape(1, D, HEADS_WIDTH), scale


def solution(mesh):
    return jax.shard_map(shards, mesh=mesh, in_specs=(P(("gx", "ta")),), out_specs=(P(None, None, "ta"), P(None, "ta")), check_vma=False)
```

```python
import functools

import jax
import jax.numpy as jnp
from jax import lax
from jax.experimental import pallas as pl
from jax.experimental.pallas import tpu as pltpu
from jax.sharding import PartitionSpec as P

D = 8192
HEADS_WIDTH = 128
X, Y, Z = 4, 8, 8
ROWS = 16
HALF = Z * ROWS
A_END, LATE = 2, 4
MESH = pl.DeviceIdType.MESH


def rank(at, size):
    return jnp.where(at * 2 <= size, jnp.maximum(2 * at - 1, 0), 2 * (size - at))


def order_of(step, size):
    return lax.rem(jnp.where(step % 2 == 1, (step + 1) // 2, size - step // 2), size)


def gather_kernel(x_hbm, out_ref, scale_ref, stage, rounded, load_sem, entered_z, entered, swap_send, swap_recv, send_sem, a_recv, b_recv, late_recv, core_send, core_recv, core_late):
    gx, z = lax.axis_index("gx"), lax.axis_index("ta")
    core, chip = lax.rem(gx, 2), gx // 2
    x, y = chip // Y, lax.rem(chip, Y)
    x_rank, y_rank = rank(x, X), rank(y, Y)

    load = pltpu.make_async_copy(x_hbm, stage, load_sem)
    load.start()

    barrier = pltpu.get_barrier_semaphore()

    def device(xt, yt, zt, ct):
        return ((xt * Y + yt) * 2 + ct, zt)

    def signal(semaphore, to):
        pl.semaphore_signal(semaphore, inc=1, device_id=to, device_id_type=MESH)

    def around(size, at, then):
        for d in range(1, size):
            then(lax.rem(at + d, size))

    def greet(later, to):
        @pl.when(later)
        def _():
            signal(barrier, to)

    greet(core == 1, device(x, y, z, 1 - core))
    around(Z, z, lambda zt: greet(zt > z, device(x, y, zt, core)))
    around(Y, y, lambda yt: greet(rank(yt, Y) > y_rank, device(x, yt, z, core)))
    around(X, x, lambda xt: greet(rank(xt, X) > x_rank, device(xt, y, z, core)))

    def rows_of(xt, yt, ct, offset, count):
        start = ((xt * Y + yt) * 2 + ct) * HALF + offset
        return pl.ds(pl.multiple_of(start, ROWS), count)

    def wait_for(semaphore, count):
        @pl.when(count > 0)
        def _():
            pl.semaphore_wait(semaphore, count)

    wait_for(barrier, (1 - core) + z + y_rank + x_rank)

    def answer(earlier, semaphore, to):
        @pl.when(earlier)
        def _():
            signal(semaphore, to)

    around(Z, z, lambda zt: answer(zt < z, entered_z.at[z], device(x, y, zt, core)))
    around(Y, y, lambda yt: answer(rank(yt, Y) < y_rank, entered, device(x, yt, z, core)))
    around(X, x, lambda xt: answer(rank(xt, X) < x_rank, entered, device(xt, y, z, core)))
    answer(core == 0, entered, device(x, y, z, 1 - core))

    load.wait()
    for k in range(Z):
        rounded[k] = stage[pl.ds(k, ROWS, stride=Z), :].astype(jnp.bfloat16)
    here = rows_of(x, y, core, z * ROWS, ROWS)
    out_ref[here, :] = rounded[z]

    def remote(src, dst, send, recv, to):
        return pltpu.make_async_remote_copy(src_ref=src, dst_ref=dst, send_sem=send, recv_sem=recv, device_id=to, device_id_type=MESH)

    def swap(zt):
        @pl.when(zt > z)
        def _():
            pl.semaphore_wait(entered_z.at[zt], 1)

        remote(rounded.at[zt], out_ref.at[here], swap_send, swap_recv.at[z], device(x, y, zt, core)).start()

    def swap_soon(zt, carry):
        @pl.when((zt != z) & ((zt < z) | (zt < LATE)))
        def _():
            swap(zt)

        return carry

    def swap_rest(zt, carry):
        @pl.when(zt > z)
        def _():
            swap(zt)

        return carry

    def waiter(ref, sem):
        pltpu.make_async_copy(ref, ref, sem).wait()

    def swapped(zt, carry):
        @pl.when(zt != z)
        def _():
            waiter(rounded.at[zt], swap_recv.at[zt])

        return carry

    def along_y(ref, recv):
        for d in (1, 7, 2, 6, 3, 5, 4):
            remote(ref, ref, send_sem, recv, device(x, lax.rem(y + d, Y), z, core)).start()

    def along_x(ref, recv):
        for d in (2, 1, 3):
            remote(ref, ref, send_sem, recv, device(lax.rem(x + d, X), y, z, core)).start()

    def across(ref, recv):
        remote(ref, ref, core_send, recv, device(x, y, z, 1 - core)).start()

    def part_a(xt, yt):
        return out_ref.at[rows_of(xt, yt, core, 0, A_END * ROWS)]

    def part_b(xt, yt):
        return out_ref.at[rows_of(xt, yt, core, A_END * ROWS, (LATE - A_END) * ROWS)]

    def part_late(xt, yt):
        return out_ref.at[rows_of(xt, yt, core, LATE * ROWS, (Z - LATE) * ROWS)]

    def early(xt, yt):
        return out_ref.at[rows_of(xt, yt, core, 0, LATE * ROWS)]

    def own_a():
        lax.fori_loop(0, A_END, swapped, 0)
        along_x(part_a(x, y), a_recv.at[chip])
        along_y(part_a(x, y), a_recv.at[chip])

    def own_b():
        lax.fori_loop(A_END, LATE, swapped, 0)
        along_y(part_b(x, y), b_recv.at[chip])
        along_x(part_b(x, y), b_recv.at[chip])
        across(early(x, y), core_recv)

    def own_late():
        lax.fori_loop(LATE, Z, swapped, 0)
        along_y(part_late(x, y), late_recv.at[chip])
        along_x(part_late(x, y), late_recv.at[chip])
        across(part_late(x, y), core_late)

    def forward(part, recv, step, over_x):
        xt, yt = (order_of(step, X), y) if over_x else (x, order_of(step, Y))

        @pl.when((xt != x) | (yt != y))
        def _():
            ref, sem = part(xt, yt), recv.at[xt * Y + yt]
            waiter(ref, sem)
            (along_y if over_x else along_x)(ref, sem)
            if part is part_late:
                across(ref, core_late)

        return 0

    from_x = lambda step, carry: forward(part_a, a_recv, step, True)
    from_y = lambda step, carry: forward(part_b, b_recv, step, False)
    late_from_y = lambda step, carry: forward(part_late, late_recv, step, False)
    def loop(start, end, body):
        lax.fori_loop(start, end, body, 0)

    loop(0, Z, swap_soon)

    @pl.when(z < LATE)
    def _():
        wait_for(entered, (Y - 1 - y_rank) + (X - 1 - x_rank) + core)
        own_a()
        loop(LATE, Z, swap_rest)
        own_b()
        own_late()
        loop(0, 3, from_x)
        loop(0, Y, from_y)
        loop(3, X, from_x)
        loop(0, Y, late_from_y)

    @pl.when(z >= LATE)
    def _():
        loop(LATE, Z, swap_rest)
        wait_for(entered, (Y - 1 - y_rank) + (X - 1 - x_rank) + core)
        own_late()
        own_a()
        own_b()
        loop(0, X, from_x)
        loop(0, Y, late_from_y)
        loop(0, Y, from_y)

    def arrival(step, carry):
        xt, yt = order_of(step // 8, X), order_of(lax.rem(step, 8), Y)
        source = xt * Y + yt

        @pl.when(source != chip)
        def _():
            @pl.when(yt != y)
            def _():
                waiter(part_a(xt, yt), a_recv.at[source])

            @pl.when(xt != x)
            def _():
                waiter(part_b(xt, yt), b_recv.at[source])

            across(early(xt, yt), core_recv)

        return carry

    def late_arrival(step, carry):
        xt, yt = order_of(step // 8, X), order_of(lax.rem(step, 8), Y)
        source = xt * Y + yt

        @pl.when(source != chip)
        def _():
            @pl.when(xt != x)
            def _():
                waiter(part_late(xt, yt), late_recv.at[source])
                across(part_late(xt, yt), core_late)

        return carry

    lax.fori_loop(0, X * Y, arrival, 0)
    lax.fori_loop(0, X * Y, late_arrival, 0)

    def largest(ct, offset, count, best):
        def step(p, best):
            block = jnp.abs(out_ref[pl.ds(pl.multiple_of((p * 2 + ct) * HALF + offset, ROWS), count), :])
            return jnp.maximum(best, jnp.max(block.reshape(count // 32, 32, HEADS_WIDTH), axis=0))

        return lax.fori_loop(0, X * Y, step, best, unroll=4)

    best = largest(core, 0, HALF, jnp.zeros((32, HEADS_WIDTH), jnp.bfloat16))
    waiter(out_ref.at[pl.ds(0, X * Y * LATE * ROWS)], core_recv)
    best = largest(1 - core, 0, LATE * ROWS, best)
    waiter(out_ref.at[pl.ds(0, X * Y * (Z - LATE) * ROWS)], core_late)
    best = largest(1 - core, LATE * ROWS, (Z - LATE) * ROWS, best)
    scale_ref[...] = jnp.max(best.astype(jnp.float32), axis=0, keepdims=True)
    waiter(out_ref.at[pl.ds(0, (Z - 1) * ROWS)], swap_send)
    a_rows, b_rows = A_END * ROWS, (Z - A_END) * ROWS
    sent = a_rows * ((X - 1) + X * (Y - 1)) + b_rows * ((Y - 1) + Y * (X - 1))
    waiter(out_ref.at[pl.ds(0, sent)], send_sem)
    waiter(out_ref.at[pl.ds(0, D // 2)], core_send)


TILES = (512, 512, 1024, 1024, 1024, 1024, 1024, 1024, 512, 512)


def scale_kernel(w_ref, scale_ref, out_hbm, scale_hbm, buffer, out_sem, scale_sem):
    scale_out = pltpu.make_async_copy(scale_ref, scale_hbm, scale_sem)
    scale_out.start()
    inverse = jnp.broadcast_to(1.0 / scale_ref[...], (64, HEADS_WIDTH))
    copies, start = [], 0
    for t, tile in enumerate(TILES):
        def scaled(i, carry, start=start):
            rows = pl.ds(pl.multiple_of(start + i * 64, 64), 64)
            buffer[rows, :] = (w_ref[rows, :].astype(jnp.float32) * inverse).astype(jnp.bfloat16)
            return carry

        lax.fori_loop(0, tile // 64, scaled, 0, unroll=4)
        rows = pl.ds(start, tile)
        copies.append(pltpu.make_async_copy(buffer.at[rows], out_hbm.at[rows], out_sem.at[t]))
        copies[-1].start()
        start += tile
    for copy in copies:
        copy.wait()
    scale_out.wait()


def shards(master_flat):
    flat = pltpu.with_memory_space_constraint(master_flat.reshape(ROWS * Z, HEADS_WIDTH), pltpu.HBM)
    gathered, largest = pl.pallas_call(
        gather_kernel,
        name="gather",
        out_shape=(jax.ShapeDtypeStruct((D, HEADS_WIDTH), jnp.bfloat16), jax.ShapeDtypeStruct((1, HEADS_WIDTH), jnp.float32)),
        in_specs=[pl.BlockSpec(memory_space=pltpu.HBM)],
        out_specs=(pl.BlockSpec(memory_space=pltpu.VMEM), pl.BlockSpec(memory_space=pltpu.VMEM)),
        scratch_shapes=[
            pltpu.VMEM((ROWS * Z, HEADS_WIDTH), jnp.float32),
            pltpu.VMEM((Z, ROWS, HEADS_WIDTH), jnp.bfloat16),
            pltpu.SemaphoreType.DMA,
            pltpu.SemaphoreType.REGULAR((Z,)),
            pltpu.SemaphoreType.REGULAR,
            pltpu.SemaphoreType.DMA,
            pltpu.SemaphoreType.DMA((Z,)),
            pltpu.SemaphoreType.DMA,
            pltpu.SemaphoreType.DMA((X * Y,)),
            pltpu.SemaphoreType.DMA((X * Y,)),
            pltpu.SemaphoreType.DMA((X * Y,)),
            pltpu.SemaphoreType.DMA,
            pltpu.SemaphoreType.DMA,
            pltpu.SemaphoreType.DMA,
        ],
        compiler_params=pltpu.CompilerParams(collective_id=0, has_side_effects=True, vmem_limit_bytes=16 * 1024 * 1024),
    )(flat)
    weight, scale = pl.pallas_call(
        scale_kernel,
        name="scale",
        out_shape=(jax.ShapeDtypeStruct((D, HEADS_WIDTH), jnp.bfloat16), jax.ShapeDtypeStruct((1, HEADS_WIDTH), jnp.float32)),
        in_specs=[pl.BlockSpec(memory_space=pltpu.VMEM), pl.BlockSpec(memory_space=pltpu.VMEM)],
        out_specs=(pl.BlockSpec(memory_space=pl.ANY), pl.BlockSpec(memory_space=pl.ANY)),
        scratch_shapes=[
            pltpu.VMEM((D, HEADS_WIDTH), jnp.bfloat16),
            pltpu.SemaphoreType.DMA((len(TILES),)),
            pltpu.SemaphoreType.DMA,
        ],
        compiler_params=pltpu.CompilerParams(vmem_limit_bytes=16 * 1024 * 1024),
    )(gathered, largest)
    return weight.reshape(1, D, HEADS_WIDTH), scale


def solution(mesh):
    return jax.shard_map(shards, mesh=mesh, in_specs=(P(("gx", "ta")),), out_specs=(P(None, None, "ta"), P(None, "ta")), check_vma=False)
```
